32 devices in a mesh: row: 8 (over z, core), col: 4 (over y, x).
Axes of the slice: x: 2, y: 2, z: 4, core: 2. Of those that a mesh axis runs over, the one named last changes fastest.
Arguments:
- tensor: bfloat16 [512, 2048, 256], P(('row', 'col')), may hold values from -6 to 6
- factor_one: bfloat16 [512, 64], P(('row', 'col')), may hold values from -0.25 to 0.25
- factor_two: bfloat16 [2048, 64], P('col'), may hold values from -0.125 to 0.125
Outputs:
- gram: float32 [256, 256], replicated
The draws below stay inside these ranges and needn't reach their ends.
All inputs are finite; a program needn't handle non-finite values.
Results may differ from the reference program's by a relative error of at most 0.0003.
Values may be sent and summed in bfloat16 or wider, within the bound.
A program may use at most 64 MiB of HBM per device.

```python
import jax
import jax.numpy as jnp
from jax import lax

SLAB = 16
I2 = 2048
I3 = 256
R1 = 64
R2 = 64
I1 = 512
N_ROW = 8
N_COL = 4


def steps_of(rng, shape, cuts, least, largest):
    def one(position, shards_of):
        draws = jax.random.uniform(jax.random.fold_in(jax.random.fold_in(rng, 6), position), (shards_of,), jnp.float32, least / len(cuts), largest / len(cuts))
        return jnp.repeat(jnp.exp(draws), shape[position] // shards_of).reshape((-1,) + (1,) * (len(shape) - position - 1))

    gain = one(*cuts[0])
    for cut in cuts[1:]:
        gain = gain * one(*cut)
    return gain


def noise(key, extent, width, limit, cuts=(), held_as=jnp.bfloat16):
    entries = jax.random.normal(key, extent, jnp.float32) * width
    if len(cuts) > 0:
        entries = steps_of(key, extent, cuts, -0.22, 0.18) * entries
    return jnp.clip(entries, min=-limit, max=limit).astype(held_as)


def setup_inputs(seed: int = 0) -> dict:
    seeds = jax.random.split(jax.random.key(seed), 4)
    return {
        "tensor": noise(seeds[0], (I1, I2, I3), 1.0, 6.0, ((0, 32),)),
        "factor_one": noise(seeds[1], (I1, R1), I1 ** -0.5, 0.25, ((0, 32),)),
        "factor_two": noise(seeds[2], (I2, R2), I2 ** -0.5, 0.125, ((0, 4),)),
    }


def reference(tensor, factor_one, factor_two):
    slabs = tensor.reshape(N_ROW * N_COL, SLAB, I2, I3)
    rows_one = factor_one.reshape(N_ROW * N_COL, SLAB, R1)
    second = factor_two.astype(jnp.float32)

    def absorb(carry, pieces):
        block, first = pieces
        partly = jnp.einsum("abk,br->ark", block.astype(jnp.float32), second, precision=lax.Precision.HIGHEST)
        core = jnp.einsum("ark,as->srk", partly, first.astype(jnp.float32), precision=lax.Precision.HIGHEST)
        return carry + core, None

    start = jnp.zeros((R1, R2, I3), jnp.float32)
    core, unused = lax.scan(absorb, start, (slabs, rows_one))
    flat = core.reshape(R1 * R2, I3)
    gram = jnp.dot(flat.T, flat, precision=lax.Precision.HIGHEST, preferred_element_type=jnp.float32)
    return gram / (R1 * R2)
```

```python
import functools

import jax
import jax.numpy as jnp
from jax import lax
from jax.experimental import pallas as pl
from jax.experimental.pallas import tpu as pltpu
from jax.sharding import PartitionSpec as P

MESH = pl.DeviceIdType.MESH
F32 = jnp.float32
BF16 = jnp.bfloat16
TILE = 8


def over_rows(left, right):
    return lax.dot_general(
        left, right, (((0,), (0,)), ((), ())), preferred_element_type=F32
    )


def split(x):
    high = x.astype(BF16)
    return high, (x - high.astype(F32)).astype(BF16)


def kernel(
    n_col, n, share, copies, owners,
    t_ref, f1_ref, f2_ref, out_ref,
    held, twos, ones, ones_all, stage, recv, part, part_all, total,
    load_sem, two_send, two_recv, one_send, one_recv,
    mid_send, mid_recv, part_send, part_recv, all_send, all_recv,
):
    slab, rank_one = f1_ref.shape
    rank_two = f2_ref.shape[0]
    chunks = stage.shape[1]
    per_chunk = slab // chunks
    my_row, my_col = lax.axis_index("row"), lax.axis_index("col")
    me = my_row * n_col + my_col

    def load(c):
        rows = pl.ds(c * per_chunk, per_chunk)
        return pltpu.make_async_copy(t_ref.at[rows], held.at[rows], load_sem.at[c])

    for c in range(chunks):
        load(c).start()

    barrier = pltpu.get_barrier_semaphore()

    def greet(off, _):
        d = lax.rem(me + off, n)
        pl.semaphore_signal(
            barrier, inc=1, device_id=(d // n_col, lax.rem(d, n_col)), device_id_type=MESH
        )
        return 0

    lax.fori_loop(1, n, greet, 0)

    spread_rows, width = ones.shape
    iota = lambda shape, dim: lax.broadcasted_iota(jnp.int32, shape, dim)
    lanes = iota((rank_one, width), 1)
    repeat = (lax.rem(lanes, rank_one) == iota((rank_one, width), 0)).astype(BF16)
    wide = jnp.dot(f1_ref[...], repeat, preferred_element_type=F32).astype(BF16)
    tall = (iota((spread_rows, slab), 0) // share == iota((spread_rows, slab), 1)).astype(BF16)
    spread = jnp.dot(tall, wide, preferred_element_type=F32)
    keep = iota((spread_rows, width), 1) // rank_one == lax.rem(iota((spread_rows, width), 0), share)
    ones[...] = jnp.where(keep, spread, 0.0).astype(BF16)
    ones_all[me] = ones[...]
    twos[my_col] = f2_ref[...]

    pl.semaphore_wait(barrier, n - 1)

    for off in range(1, n_col):
        pltpu.make_async_remote_copy(
            src_ref=f2_ref, dst_ref=twos.at[my_col],
            send_sem=two_send, recv_sem=two_recv,
            device_id=(my_row, lax.rem(my_col + off, n_col)), device_id_type=MESH,
        ).start()

    def to_all(src, dst, send_sem, recv_sem):
        def one(off, _):
            d = lax.rem(me + off, n)
            pltpu.make_async_remote_copy(
                src_ref=src(d), dst_ref=dst, send_sem=send_sem, recv_sem=recv_sem,
                device_id=(d // n_col, lax.rem(d, n_col)), device_id_type=MESH,
            ).start()
            return 0

        lax.fori_loop(1, n, one, 0)

    def wait_bytes(ref, sem):
        pltpu.make_async_copy(ref, ref, sem).wait()

    to_all(lambda d: ones, ones_all.at[me], one_send, one_recv)
    if n_col > 1:
        wait_bytes(twos.at[pl.ds(0, n_col - 1)], two_recv)
    second = jnp.concatenate([twos[q] for q in range(n_col)], axis=1)

    for c in range(chunks):
        load(c).wait()
        for i in range(per_chunk):
            partly = jnp.dot(second, held[c * per_chunk + i], preferred_element_type=F32)
            for b in range(rank_two // share):
                stage[b, c, pl.ds(i * share, share), :] = partly[b * share:(b + 1) * share, :]
        to_all(lambda d: stage.at[d // copies, c], recv.at[me, c], mid_send, mid_recv)

    recv[me] = stage[me // copies]
    wait_bytes(ones_all.at[pl.ds(0, n - 1)], one_recv)
    wait_bytes(recv.at[pl.ds(0, n - 1)], mid_recv)

    depth = recv.shape[3]
    first = ones_all[...].reshape(n * spread_rows, width)
    high, low = split(recv[...].reshape(n * spread_rows, depth))
    flat = over_rows(first, high) + over_rows(first, low)
    if copies > 1:
        mine = iota(flat.shape, 0) // (rank_one // copies) == lax.rem(me, copies)
        flat = jnp.where(mine, flat, 0.0)
    high, low = split(flat)
    gram = over_rows(high, high) + over_rows(high, low) + over_rows(low, high)
    part[...] = gram.reshape(part.shape)

    def send_part(off, _):
        d = lax.rem(me + off, n)

        @pl.when(d < owners)
        def _():
            pltpu.make_async_remote_copy(
                src_ref=part.at[d], dst_ref=part_all.at[me],
                send_sem=part_send, recv_sem=part_recv,
                device_id=(d // n_col, lax.rem(d, n_col)), device_id_type=MESH,
            ).start()

        return 0

    lax.fori_loop(1, n, send_part, 0)

    @pl.when(me < owners)
    def _():
        part_all[me] = part[me]
        wait_bytes(part_all.at[pl.ds(0, n - 1)], part_recv)
        total[me] = jnp.sum(part_all[...], axis=0)
        to_all(lambda d: total.at[me], total.at[me], all_send, all_recv)
        wait_bytes(total.at[pl.ds(0, owners - 1)], all_recv)
        wait_bytes(part.at[pl.ds(0, owners - 1)], part_send)
        wait_bytes(part_all.at[pl.ds(0, n - 1)], all_send)

    if owners < n:
        @pl.when(me >= owners)
        def _():
            wait_bytes(total, all_recv)
            wait_bytes(part, part_send)

    out_ref[...] = total[...].reshape(out_ref.shape)
    if n_col > 1:
        wait_bytes(twos.at[pl.ds(0, n_col - 1)], two_send)
    wait_bytes(ones_all.at[pl.ds(0, n - 1)], one_send)
    wait_bytes(recv.at[pl.ds(0, n - 1)], mid_send)


def per_device(n_row, n_col, tensor, factor_one, factor_two):
    slab, second_size, depth = tensor.shape
    rank_one, rank_two = factor_one.shape[1], factor_two.shape[1]
    n = n_row * n_col
    share = max(1, rank_two // n)
    copies = max(1, n // rank_two)
    owners = min(n, depth // TILE)
    rows = depth // owners
    chunks = slab * share // TILE
    width = max(128, share * rank_one)
    dma = pltpu.SemaphoreType.DMA
    gram = pl.pallas_call(
        functools.partial(kernel, n_col, n, share, copies, owners),
        out_shape=jax.ShapeDtypeStruct((depth, depth), F32),
        in_specs=[
            pl.BlockSpec(memory_space=pl.ANY),
            pl.BlockSpec(memory_space=pltpu.VMEM),
            pl.BlockSpec(memory_space=pltpu.VMEM),
        ],
        out_specs=pl.BlockSpec(memory_space=pltpu.VMEM),
        scratch_shapes=[
            pltpu.VMEM(tensor.shape, BF16),
            pltpu.VMEM((n_col, rank_two, second_size // n_col), BF16),
            pltpu.VMEM((slab * share, width), BF16),
            pltpu.VMEM((n, slab * share, width), BF16),
            pltpu.VMEM((rank_two // share, chunks, TILE, depth), F32),
            pltpu.VMEM((n, chunks, TILE, depth), F32),
            pltpu.VMEM((owners, rows, depth), F32),
            pltpu.VMEM((n, rows, depth), F32),
            pltpu.VMEM((owners, rows, depth), F32),
            dma((chunks,)),
        ] + [dma] * 10,
        compiler_params=pltpu.CompilerParams(
            collective_id=0, has_side_effects=True, vmem_limit_bytes=60 * 2**20
        ),
        name="project_and_gram",
    )(tensor, factor_one, factor_two.T)
    return gram / (rank_one * rank_two)


def solution(mesh):
    sizes = mesh.shape
    placed = (P(("row", "col"), None, None), P(("row", "col"), None), P("col", None))
    return jax.shard_map(
        functools.partial(per_device, sizes["row"], sizes["col"]),
        mesh=mesh, in_specs=placed, out_specs=P(), check_vma=False,
    )
```

```python
import functools

import jax
import jax.numpy as jnp
from jax import lax
from jax.experimental import pallas as pl
from jax.experimental.pallas import tpu as pltpu
from jax.sharding import PartitionSpec as P

MESH = pl.DeviceIdType.MESH
F32 = jnp.float32
BF16 = jnp.bfloat16
TILE = 8


def over_rows(left, right):
    return lax.dot_general(
        left, right, (((0,), (0,)), ((), ())), preferred_element_type=F32
    )


def split(x):
    high = x.astype(BF16)
    return high, (x - high.astype(F32)).astype(BF16)


def kernel(
    n_row, n_col, share,
    t_ref, f1_ref, f2_ref, out_ref,
    held, twos, ones, ones_all, spread, stage, recv, outbox, inbox, part, part_all, lines, total,
    load_sem, two_send, two_recv, one_send, one_recv,
    mid_send, mid_recv, box_send, box_recv, part_send, part_recv, line_send, line_recv, all_send, all_recv,
):
    slab, rank_one = f1_ref.shape
    rank_two = f2_ref.shape[0]
    chunks, depth = stage.shape[1], stage.shape[3]
    rows = slab * share
    per_chunk = slab // chunks
    my_row, my_col = lax.axis_index("row"), lax.axis_index("col")
    half_rows = n_row // 2
    n = half_rows * n_col
    my_half, my_seat = my_row // half_rows, lax.rem(my_row, half_rows)
    me = my_seat * n_col + my_col

    def place(d):
        return my_half * half_rows + d // n_col, lax.rem(d, n_col)


    def load(c):
        rows = pl.ds(c * per_chunk, per_chunk)
        return pltpu.make_async_copy(t_ref.at[rows], held.at[rows], load_sem.at[c])

    for c in range(chunks):
        load(c).start()

    barrier = pltpu.get_barrier_semaphore()

    def greet(off, _):
        d = lax.rem(my_row * n_col + my_col + off, 2 * n)
        pl.semaphore_signal(
            barrier, inc=1, device_id=(d // n_col, lax.rem(d, n_col)), device_id_type=MESH
        )
        return 0

    lax.fori_loop(1, 2 * n, greet, 0)

    iota = lambda shape, dim: lax.broadcasted_iota(jnp.int32, shape, dim)
    folds = slab // ones.shape[0]
    ones[...] = jnp.concatenate(
        [f1_ref[pl.ds(q * ones.shape[0], ones.shape[0]), :] for q in range(folds)], axis=1
    )
    ones_all[me] = ones[...]
    twos[my_col] = f2_ref[...]

    pl.semaphore_wait(barrier, 2 * n - 1)

    for off in range(1, n_col):
        pltpu.make_async_remote_copy(
            src_ref=f2_ref, dst_ref=twos.at[my_col],
            send_sem=two_send, recv_sem=two_recv,
            device_id=(my_row, lax.rem(my_col + off, n_col)), device_id_type=MESH,
        ).start()

    def to_all(src, dst, send_sem, recv_sem):
        def one(off, _):
            d = lax.rem(me + off, n)
            pltpu.make_async_remote_copy(
                src_ref=src(d), dst_ref=dst, send_sem=send_sem, recv_sem=recv_sem,
                device_id=place(d), device_id_type=MESH,
            ).start()
            return 0

        lax.fori_loop(1, n, one, 0)

    def wait_bytes(ref, sem):
        pltpu.make_async_copy(ref, ref, sem).wait()

    to_all(lambda d: ones, ones_all.at[me], one_send, one_recv)
    if n_col > 1:
        wait_bytes(twos.at[pl.ds(0, n_col - 1)], two_recv)
    second = jnp.concatenate([twos[q] for q in range(n_col)], axis=1)

    for c in range(chunks):
        load(c).wait()
        for i in range(per_chunk):
            partly = jnp.dot(second, held[c * per_chunk + i], preferred_element_type=F32)
            for b in range(rank_two // share):
                stage[b, c, pl.ds(i * share, share), :] = partly[b * share:(b + 1) * share, :]
        landing = recv.at[pl.ds(pl.multiple_of(me * rows + c * TILE, TILE), TILE)]
        to_all(lambda d: stage.at[d, c], landing, mid_send, mid_recv)

    recv[pl.ds(pl.multiple_of(me * rows, TILE), rows), :] = stage[me].reshape(rows, depth)
    wait_bytes(ones_all.at[pl.ds(0, n - 1)], one_recv)
    packed = ones_all[...].astype(F32)
    whole = jnp.concatenate(
        [packed[:, :, q * rank_one:(q + 1) * rank_one] for q in range(folds)], axis=1
    ).reshape(n * slab, rank_one)
    for j in range(share):
        for w in range(spread.shape[0]):
            parts = [
                whole if w * folds + p == j else jnp.zeros_like(whole) for p in range(folds)
            ]
            spread[w, pl.ds(j, n * slab, stride=share), :] = jnp.concatenate(parts, axis=1)
    first = jnp.concatenate([spread[w] for w in range(spread.shape[0])], axis=1).astype(BF16)
    wait_bytes(recv.at[pl.ds(0, (n - 1) * rows)], mid_recv)

    high, low = split(recv[...])
    flat = over_rows(first, high) + over_rows(first, low)
    outbox[...] = flat[:share * rank_one].reshape(outbox.shape)
    swap = pltpu.make_async_remote_copy(
        src_ref=outbox.at[1 - my_half], dst_ref=inbox, send_sem=box_send, recv_sem=box_recv,
        device_id=(lax.rem(my_row + half_rows, n_row), my_col), device_id_type=MESH,
    )
    swap.start()
    swap.wait_recv()
    flat = outbox[my_half] + inbox[...]
    high, low = split(flat)
    gram = over_rows(high, high) + over_rows(high, low) + over_rows(low, high)
    half = depth // 2
    part[...] = jnp.concatenate(
        [gram[:half, :half], gram[:half, half:], gram[half:, half:]], axis=0
    ).reshape(part.shape)

    plane, planes = part.shape[0], lines.shape[0]
    core, line = lax.rem(my_row, 2), my_row // 2
    seat = core * n_col + my_col

    def mate(off):
        other = lax.rem(seat + off, plane)
        return other, (line * 2 + other // n_col, lax.rem(other, n_col))

    def send(src, dst, send_sem, recv_sem, device):
        pltpu.make_async_remote_copy(
            src_ref=src, dst_ref=dst, send_sem=send_sem, recv_sem=recv_sem,
            device_id=device, device_id_type=MESH,
        ).start()

    for off in range(1, plane):
        other, device = mate(off)
        send(part.at[other], part_all.at[seat], part_send, part_recv, device)
    part_all[seat] = part[seat]
    wait_bytes(part_all.at[pl.ds(0, plane - 1)], part_recv)
    lines[line] = jnp.sum(part_all[...], axis=0)
    for off in range(1, planes):
        device = (lax.rem(line + off, planes) * 2 + core, my_col)
        send(lines.at[line], lines.at[line], line_send, line_recv, device)
    if planes > 1:
        wait_bytes(lines.at[pl.ds(0, planes - 1)], line_recv)
    total[seat] = jnp.sum(lines[...], axis=0)
    for off in range(1, plane):
        _, device = mate(off)
        send(total.at[seat], total.at[seat], all_send, all_recv, device)
    wait_bytes(total.at[pl.ds(0, plane - 1)], all_recv)

    blocks = total[...].reshape(3, half, half)
    out_ref[:half, :half] = blocks[0]
    out_ref[:half, half:] = blocks[1]
    out_ref[half:, :half] = blocks[1].T
    out_ref[half:, half:] = blocks[2]
    swap.wait_send()
    wait_bytes(part_all.at[pl.ds(0, plane - 1)], part_send)
    if planes > 1:
        wait_bytes(lines.at[pl.ds(0, planes - 1)], line_send)
    wait_bytes(total.at[pl.ds(0, plane - 1)], all_send)
    if n_col > 1:
        wait_bytes(twos.at[pl.ds(0, n_col - 1)], two_send)
    wait_bytes(ones_all.at[pl.ds(0, n - 1)], one_send)
    wait_bytes(recv.at[pl.ds(0, (n - 1) * rows)], mid_send)


def per_device(n_row, n_col, tensor, factor_one, factor_two):
    slab, second_size, depth = tensor.shape
    rank_one, rank_two = factor_one.shape[1], factor_two.shape[1]
    n = n_row // 2 * n_col
    share = rank_two // n
    plane, planes = 2 * n_col, n_row // 2
    half = depth // 2
    block = (3 * half // plane, half)
    chunks = slab * share // TILE
    packed = (slab * rank_one // 128, 128)
    dma = pltpu.SemaphoreType.DMA
    gram = pl.pallas_call(
        functools.partial(kernel, n_row, n_col, share),
        out_shape=jax.ShapeDtypeStruct((depth, depth), F32),
        in_specs=[
            pl.BlockSpec(memory_space=pl.ANY),
            pl.BlockSpec(memory_space=pltpu.VMEM),
            pl.BlockSpec(memory_space=pltpu.VMEM),
        ],
        out_specs=pl.BlockSpec(memory_space=pltpu.VMEM),
        scratch_shapes=[
            pltpu.VMEM(tensor.shape, BF16),
            pltpu.VMEM((n_col, rank_two, second_size // n_col), BF16),
            pltpu.VMEM(packed, BF16),
            pltpu.VMEM((n, *packed), BF16),
            pltpu.VMEM((-(-share * rank_one // 128), n * slab * share, 128), F32),
            pltpu.VMEM((rank_two // share, chunks, TILE, depth), F32),
            pltpu.VMEM((n * slab * share, depth), F32),
            pltpu.VMEM((2, share * rank_one // 2, depth), F32),
            pltpu.VMEM((share * rank_one // 2, depth), F32),
            pltpu.VMEM((plane, *block), F32),
            pltpu.VMEM((plane, *block), F32),
            pltpu.VMEM((planes, *block), F32),
            pltpu.VMEM((plane, *block), F32),
            dma((chunks,)),
        ] + [dma] * 14,
        compiler_params=pltpu.CompilerParams(
            collective_id=0, has_side_effects=True, vmem_limit_bytes=60 * 2**20
        ),
        name="project_and_gram",
    )(tensor, factor_one, factor_two.T)
    return gram / (rank_one * rank_two)


def solution(mesh):
    sizes = mesh.shape
    placed = (P(("row", "col"), None, None), P(("row", "col"), None), P("col", None))
    return jax.shard_map(
        functools.partial(per_device, sizes["row"], sizes["col"]),
        mesh=mesh, in_specs=placed, out_specs=P(), check_vma=False,
    )
```
